256 devices in a mesh: grp: 4 (over x, y), ep: 64 (over z, core).
Axes of the slice: x: 2, y: 2, z: 32, core: 2. Of those that a mesh axis runs over, the one named last changes fastest.
The devices are a block of a 4x8x32 slice.
Arguments:
- expert_ids: int32 [16384, 8], P(('grp', 'ep')), parts along dimension 0, may hold values from 0 to 63, all different within a row; in each aligned block of 64 rows (0 to 63, 64 to 127, ...) at most 16 rows name the same one
- route_gates: float32 [16384, 8], P(('grp', 'ep')), parts along dimension 0, may hold values from 0.1 to 0.5
- routed_in: bfloat16 [16384, 8, 2048], P(('grp', 'ep')), parts along dimension 0, may hold values from -6 to 6
- down_weight: bfloat16 [64, 1024, 3584], P('ep'), may hold values from -0.1875 to 0.1875
- slot_offset: int32 [1], replicated, may hold values from 0 to 63
Outputs:
- combined: bfloat16 [16384, 3584], P(('grp', 'ep')), parts along dimension 0
The draws below stay inside these ranges and needn't reach their ends.
There are 4 independent parts, one for each index of `grp`. The reference program is written for one: setup_inputs(seed, part) draws one part's arguments, and reference() takes and returns one part's arrays. A program takes and returns all parts, laid end to end along the dimension named above; an argument that names none is the same for every part. Nothing has to cross between parts.
Inputs may be any that keep to these rules, and one draw needn't show every extreme that they name: `expert_ids`: each row names 8 different experts. Among the tokens of one ep device, no expert is named by more than 16 tokens, a bound that some block reaches in some devices.
All inputs are finite; a program needn't handle non-finite values.
Results may differ from the reference program's by a relative error of at most 0.0057.
Values may be sent and summed in bfloat16 or wider, within the bound.
No kernel may reach another device: no remote copies, remote signals or barrier semaphores. Data moves between devices by JAX's collectives and lax.ppermute only.
A program may use at most 128 MiB of HBM per device.

```python
import math
import jax
import jax.numpy as jnp
import numpy as np
from jax import lax

D = 3584
F = 1024
TOP = 8
TOK_DEV = 64
EXPERTS = 64
TOKENS = 4096
CAP = 16


def levels(stream_key, extent, split, smallest, largest):
    loudness = 1.0
    for dim, blocks in split:
        heights = jax.random.uniform(jax.random.fold_in(jax.random.fold_in(stream_key, 6), dim), (blocks,), jnp.float32, smallest / len(split), largest / len(split))
        loudness = loudness * jnp.repeat(jnp.exp(heights), extent[dim] // blocks).reshape((-1,) + (1,) * (len(extent) - 1 - dim))
    return loudness


def routed_block(rng, own, number, rows, amount, top, most, lean):
    ranking = jax.random.permutation(rng, amount)
    crowded, ordinary = portions_of(amount, rows * top, most, lean, True), portions_of(amount, rows * top, most, lean, False)
    places = jnp.arange(amount)

    def named(sizes, turn):
        used = int((sizes > 0).sum())
        fixed = max(1, used // 4)
        moved = fixed + (places - fixed + turn * (used - fixed)) % max(1, amount - fixed)
        return jnp.zeros((amount,), jnp.int32).at[ranking[jnp.where(places < fixed, places, moved)]].set(jnp.asarray(sizes, jnp.int32))

    sizes = jnp.where(number % 4 == 0, named(crowded, number // 4), named(ordinary, number - number // 4 - 1))
    mixed = jax.random.permutation(jax.random.fold_in(own, 3), amount)
    giver, taker = mixed[0:amount // 2 * 2:2], mixed[1:amount // 2 * 2:2]
    margin = jnp.minimum(sizes[giver] - 1, most - sizes[taker]) // 2
    margin = jnp.where((giver == ranking[0]) | (taker == ranking[0]) | (sizes[taker] == 0), 0, jnp.maximum(margin, 0))
    moved = jax.random.randint(jax.random.fold_in(own, 4), (amount // 2,), 0, 1 << 20) % (margin + 1)
    sizes = sizes.at[giver].add(-moved).at[taker].add(moved)
    members = jnp.searchsorted(jnp.cumsum(sizes), jnp.arange(rows * top), side="right").astype(jnp.int32)
    grid = members.reshape(top, rows).T
    grid = grid[jax.random.permutation(jax.random.fold_in(own, 1), rows)]
    turn = jax.random.randint(jax.random.fold_in(own, 2), (rows, 1), 0, top)
    return jnp.take_along_axis(grid, (jnp.arange(top)[None, :] + turn) % top, axis=1)


def portions_of(number_of, total, reach, lean, full):
    portions = [(1 << 20) // math.isqrt(rank ** lean) + 1 for rank in range(1, number_of + 1)]
    largest = reach if full else min(reach, max(-(-total // number_of), total * portions[0] // sum(portions)))
    least = 1 if total - largest >= number_of - 1 else 0
    counts, rest = [largest] + [least] * (number_of - 1), total - largest - least * (number_of - 1)
    while rest > 0:
        movable = [i for i in range(1, number_of) if counts[i] < largest] or [i for i in range(1, number_of) if counts[i] < reach]
        pool, budget = sum([portions[i] for i in movable]), rest
        for i in movable:
            more = min(reach - counts[i], max(1, budget * portions[i] // pool), rest)
            counts[i] = counts[i] + more
            rest = rest - more
    return np.array(counts)


def scatter_about(stream_key, shape, spread, bound, pieces=(), kind=jnp.bfloat16):
    values = jax.random.normal(stream_key, shape, jnp.float32) * spread
    if len(pieces) > 0:
        values = levels(stream_key, shape, pieces, -0.22, 0.18) * values
    return jnp.clip(values, min=-bound, max=bound).astype(kind)


def setup_inputs(seed: int = 0, part: int = 0) -> dict:
    splits = jax.random.split(jax.random.key(seed), 6)
    part_keys = jax.random.split(jax.random.fold_in(splits[5], part), 6)
    expert_ids_keys = jax.random.split(jax.random.fold_in(part_keys[0], 1), TOKENS // TOK_DEV)
    expert_ids_turns = jax.random.permutation(jax.random.fold_in(part_keys[0], 3), TOKENS // TOK_DEV)
    expert_ids = jax.vmap(lambda own, number: routed_block(jax.random.fold_in(part_keys[0], 2), own, number, TOK_DEV, EXPERTS, TOP, CAP, 2))(expert_ids_keys, expert_ids_turns).reshape((TOKENS, TOP))
    route_gates = jnp.clip(0.1 + 0.4 * jax.random.uniform(part_keys[1], (TOKENS, TOP), jnp.float32) ** levels(part_keys[1], (TOKENS, TOP), ((0, 64),), -0.2, 0.2), 0.1, 0.5)
    routed_in = scatter_about(part_keys[2], (TOKENS, TOP, 2 * F), 1.0, 6.0, ((0, 64),))
    down_weight = scatter_about(splits[3], (EXPERTS, F, D), F ** -0.5, 0.1875, ((0, 64),))
    slot_offset = jax.random.randint(splits[4], (1,), 0, EXPERTS).astype(jnp.int32)
    return dict(expert_ids=expert_ids, route_gates=route_gates, routed_in=routed_in, down_weight=down_weight, slot_offset=slot_offset)


def swiglu(packed):
    half = packed.shape[-1] // 2
    gate = packed[..., :half].astype(jnp.float32)
    upper = packed[..., half:].astype(jnp.float32)
    return (jax.nn.silu(gate) * upper).astype(jnp.bfloat16)


def reference(expert_ids, route_gates, routed_in, down_weight, slot_offset):
    pairs = expert_ids.reshape(-1).astype(jnp.int32)
    pair_count = pairs.shape[0]
    most_rows = EXPERTS * CAP
    hidden = swiglu(routed_in).reshape(pair_count, F)
    order = jnp.argsort(pairs, stable=True).astype(jnp.int32)
    inverse = jnp.argsort(order, stable=True).astype(jnp.int32)
    sorted_hidden = jnp.concatenate([hidden[order], jnp.zeros((most_rows, F), jnp.bfloat16)], axis=0)
    loads = jnp.sum((pairs[:, None] == jnp.arange(EXPERTS, dtype=jnp.int32)[None, :]).astype(jnp.int32), axis=0)
    starts = (jnp.cumsum(loads) - loads).astype(jnp.int32)

    def one_expert(carry, expert):
        start = starts[expert]
        rows = lax.dynamic_slice_in_dim(sorted_hidden, start, most_rows, 0)
        matrix = down_weight[jnp.mod(expert - slot_offset[0], EXPERTS).astype(jnp.int32)]
        result = jnp.dot(rows, matrix, preferred_element_type=jnp.float32).astype(jnp.bfloat16)
        live = jnp.arange(most_rows, dtype=jnp.int32) < loads[expert]
        before = lax.dynamic_slice_in_dim(carry, start, most_rows, 0)
        update = jnp.where(live[:, None], result, before)
        return lax.dynamic_update_slice_in_dim(carry, update, start, 0), None

    initial = jnp.zeros((pair_count + most_rows, D), jnp.bfloat16)
    filled, unused = lax.scan(one_expert, initial, jnp.arange(EXPERTS, dtype=jnp.int32))
    outputs = filled[:pair_count][inverse].reshape(TOKENS, TOP, D)
    total = jnp.zeros((TOKENS, D), jnp.float32)
    for choice_index in range(TOP):
        total = total + route_gates[:, choice_index, None] * outputs[:, choice_index].astype(jnp.float32)
    return total.astype(jnp.bfloat16)
```

```python
import jax
import jax.numpy as jnp
from jax import lax
from jax.experimental import pallas as pl
from jax.experimental.pallas import tpu as pltpu
from jax.sharding import PartitionSpec as P

CHAINS = 2
NO_TOKEN = 1024.0
INTERPRET = False


def exact_parts(value):
    high = value.astype(jnp.bfloat16).astype(jnp.float32)
    rest = value - high
    middle = rest.astype(jnp.bfloat16).astype(jnp.float32)
    return high, middle, rest - middle


def pack_kernel(target_ref, gate_ref, routed_ref, rows_ref, meta_ref, *, experts, capacity, chosen):
    pairs, width = routed_ref.shape
    half = width // 2
    target = target_ref[...]
    expert = lax.broadcasted_iota(jnp.int32, (experts, pairs), 0)
    before = lax.broadcasted_iota(jnp.int32, (pairs, pairs), 0) < lax.broadcasted_iota(
        jnp.int32, (pairs, pairs), 1
    )
    named = expert == target
    earlier = jnp.dot(
        named.astype(jnp.bfloat16), before.astype(jnp.bfloat16), preferred_element_type=jnp.float32
    )
    rank = jnp.sum(jnp.where(named, earlier, 0.0), axis=0, keepdims=True).astype(jnp.int32)
    slot = target * capacity + rank
    at_rank = (lax.broadcasted_iota(jnp.int32, (capacity, pairs), 0) == rank).astype(jnp.bfloat16)
    token = (lax.broadcasted_iota(jnp.int32, (1, pairs), 1) // chosen + 1).astype(jnp.float32)
    values = (token,) + exact_parts(gate_ref[...])
    partner = (expert ^ 1) == target
    for place, value in enumerate(values):
        for side, mask in enumerate((named, partner)):
            found = lax.dot_general(
                jnp.where(mask, value, 0.0).astype(jnp.bfloat16),
                at_rank,
                (((1,), (1,)), ((), ())),
                preferred_element_type=jnp.float32,
            )
            if place == 0:
                found = jnp.where(found > 0.0, found - 1.0, NO_TOKEN)
            start = (2 * place + side) * capacity
            meta_ref[:, start : start + capacity] = found
    gate = routed_ref[:, :half].astype(jnp.float32)
    upper = routed_ref[:, half:].astype(jnp.float32)
    hidden = (gate / (1.0 + jnp.exp(-gate)) * upper).astype(jnp.bfloat16)
    pick = (
        lax.broadcasted_iota(jnp.int32, (experts * capacity, pairs), 0) == slot
    ).astype(jnp.bfloat16)
    rows_ref[...] = jnp.dot(pick, hidden, preferred_element_type=jnp.float32).astype(jnp.bfloat16)


def expert_kernel(place_ref, *refs, homes, chips, tokens):
    count = len(homes)
    own_rows, other_rows = refs[:count], refs[count : 2 * count]
    own_weight, other_weight, token_ref, gate_ref, out_ref = refs[2 * count :]
    capacity, width = own_rows[0].shape[1:]

    def project(blocks, weight):
        rows = jnp.concatenate([b[...].reshape(2 * capacity, width) for b in blocks], axis=0)
        return jnp.dot(rows, weight[...], preferred_element_type=jnp.float32).astype(jnp.bfloat16)

    own = project(own_rows, own_weight)
    other = project(other_rows, other_weight)
    lanes = token_ref.shape[2]
    wanted = lax.broadcasted_iota(jnp.int32, (2 * tokens, lanes), 0).astype(jnp.float32)
    for place, home in enumerate(homes):
        chip = lax.rem(place_ref[0] + (home + chips), chips)
        base = place * 2 * capacity
        rows = []
        for side in range(2):
            lo = base + side * capacity
            rows.append(own[lo : lo + capacity])
            rows.append(other[lo : lo + capacity])
        stacked = jnp.concatenate(rows * 3, axis=0)
        scale = jnp.where(token_ref[chip] == wanted, gate_ref[chip], 0.0).astype(jnp.bfloat16)
        out_ref[0, place] = jnp.dot(scale, stacked, preferred_element_type=jnp.float32).astype(
            jnp.bfloat16
        )


def expert_call(place, own, other, own_weight, other_weight, token, gate, homes, chips, tokens):
    experts, capacity, width = own.shape
    columns = own_weight.shape[1] // 2
    piece = columns // CHAINS
    count = len(homes)

    def row_spec(home):
        return pl.BlockSpec(
            (2, capacity, width), lambda j, s, home=home: (lax.rem(s[0] + (home + chips), chips), 0, 0)
        )

    weight_spec = pl.BlockSpec((width, piece), lambda j, s: (0, s[1] * CHAINS + j))
    table_spec = pl.BlockSpec(token.shape, lambda j, s: (0, 0, 0))
    grid_spec = pltpu.PrefetchScalarGridSpec(
        num_scalar_prefetch=1,
        grid=(CHAINS,),
        in_specs=[row_spec(h) for h in homes] * 2 + [weight_spec] * 2 + [table_spec] * 2,
        out_specs=pl.BlockSpec((1, count, 2 * tokens, piece), lambda j, s: (j, 0, 0, 0)),
    )
    return pl.pallas_call(
        lambda *refs: expert_kernel(*refs, homes=homes, chips=chips, tokens=tokens),
        grid_spec=grid_spec,
        out_shape=jax.ShapeDtypeStruct((CHAINS, count, 2 * tokens, piece), jnp.bfloat16),
        compiler_params=pltpu.CompilerParams(
            dimension_semantics=("arbitrary",), vmem_limit_bytes=32 * 1024 * 1024
        ),
        interpret=INTERPRET,
    )(place, *([own] * count), *([other] * count), own_weight, other_weight, token, gate)


def add_kernel(left_ref, right_ref, out_ref):
    def some(i, carry):
        at = pl.ds(pl.multiple_of(i * 16, 16), 16)
        total = left_ref[at].astype(jnp.float32) + right_ref[0, 0, at].astype(jnp.float32)
        out_ref[at] = total.astype(jnp.bfloat16)
        return carry

    lax.fori_loop(0, out_ref.shape[0] // 16, some, 0)


def add_own(arrived, batch, chain, place):
    return pl.pallas_call(
        add_kernel,
        grid=(1,),
        in_specs=[
            pl.BlockSpec(arrived.shape, lambda i: (0, 0)),
            pl.BlockSpec((1, 1) + arrived.shape, lambda i: (chain, place, 0, 0)),
        ],
        out_specs=pl.BlockSpec(arrived.shape, lambda i: (0, 0)),
        out_shape=jax.ShapeDtypeStruct(arrived.shape, jnp.bfloat16),
        compiler_params=pltpu.CompilerParams(vmem_limit_bytes=4 * 1024 * 1024),
        interpret=INTERPRET,
    )(arrived, batch)


def on_device(expert_ids, route_gates, routed_in, down_weight, slot_offset):
    experts = lax.axis_size("ep")
    chips = experts // 2
    tokens, chosen = expert_ids.shape
    pairs = tokens * chosen
    capacity = 2 * pairs // experts
    hidden_width = routed_in.shape[2] // 2
    weight = down_weight[0]
    width = weight.shape[1]
    index = lax.axis_index("ep")
    core = lax.rem(index, 2)
    place = jnp.stack([index // 2, core]).astype(jnp.int32)
    swap = [(i, i ^ 1) for i in range(experts)]
    onward = [(i, (i + 2) % experts) for i in range(experts)]
    backward = [(i, (i - 2) % experts) for i in range(experts)]

    partner_weight = lax.ppermute(weight, "ep", swap)
    target = jnp.mod(expert_ids - slot_offset[0], experts).reshape(1, pairs)
    rows, meta = pl.pallas_call(
        lambda *refs: pack_kernel(*refs, experts=experts, capacity=capacity, chosen=chosen),
        out_shape=(
            jax.ShapeDtypeStruct((experts * capacity, hidden_width), jnp.bfloat16),
            jax.ShapeDtypeStruct((experts, 8 * capacity), jnp.float32),
        ),
        compiler_params=pltpu.CompilerParams(vmem_limit_bytes=32 * 1024 * 1024),
        interpret=INTERPRET,
    )(target, route_gates.reshape(1, pairs), routed_in.reshape(pairs, 2 * hidden_width))
    meta = lax.all_to_all(meta, "ep", split_axis=0, concat_axis=0, tiled=True)
    own_rows = lax.all_to_all(
        rows.reshape(experts, capacity, hidden_width), "ep", split_axis=0, concat_axis=0, tiled=True
    )
    other_rows = lax.ppermute(own_rows, "ep", swap)

    meta = meta.reshape(chips, 2, 4, 2 * capacity).transpose(0, 2, 1, 3)
    token = meta[:, 0] + (tokens * jnp.arange(2, dtype=jnp.float32))[None, :, None]
    token = jnp.tile(token.reshape(chips, 1, 4 * capacity), (1, 1, 3))
    gate = meta[:, 1:].reshape(chips, 1, 12 * capacity)

    half = chips // 2
    batch = 4
    sums = {}
    for first in range(0, half, batch):
        homes = [half - s for s in range(first, first + batch)]
        homes += [s + 1 - half for s in range(first, first + batch)]
        out = expert_call(
            place, own_rows, other_rows, weight, partner_weight, token, gate, homes, chips, tokens
        )
        for i, home in enumerate(homes):
            sums[home] = (out, i)

    def own_sum(home, c):
        batch, i = sums[home]
        return batch[c, i]

    def with_own(arrived, home, c):
        batch, i = sums[home]
        return add_own(arrived, batch, c, i)

    ahead = [own_sum(half, c) for c in range(CHAINS)]
    behind = [own_sum(1 - half, c) for c in range(CHAINS)]
    for step in range(half):
        for c in range(CHAINS):
            ahead[c] = lax.ppermute(ahead[c], "ep", onward)
            if step < half - 1:
                behind[c] = lax.ppermute(behind[c], "ep", backward)
                ahead[c] = with_own(ahead[c], half - 1 - step, c)
            if step < half - 2:
                behind[c] = with_own(behind[c], step + 2 - half, c)

    done = jnp.concatenate(
        [
            (
                ahead[c].astype(jnp.float32)
                + behind[c].astype(jnp.float32)
                + own_sum(0, c).astype(jnp.float32)
            ).astype(jnp.bfloat16)
            for c in range(CHAINS)
        ],
        axis=1,
    ).reshape(2, tokens, width // 2)
    kept = lax.dynamic_index_in_dim(done, core, 0, keepdims=False)
    given = lax.dynamic_index_in_dim(done, 1 - core, 0, keepdims=False)
    taken = lax.ppermute(given, "ep", swap)
    low = jnp.where(core == 0, kept, taken)
    high = jnp.where(core == 0, taken, kept)
    return jnp.concatenate([low, high], axis=1)


def solution(mesh):
    placed = (
        P(("grp", "ep"), None),
        P(("grp", "ep"), None),
        P(("grp", "ep"), None, None),
        P("ep", None, None),
        P(),
    )
    return jax.shard_map(
        on_device, mesh=mesh, in_specs=placed, out_specs=P(("grp", "ep"), None), check_vma=False
    )
```

```python
import jax
import jax.numpy as jnp
from jax import lax
from jax.experimental import pallas as pl
from jax.experimental.pallas import tpu as pltpu
from jax.sharding import PartitionSpec as P

CHAINS = 2
BATCH = 4
INTERPRET = False


def strictly_before(size):
    earlier = lax.broadcasted_iota(jnp.int32, (size, size), 0)
    return (earlier < lax.broadcasted_iota(jnp.int32, (size, size), 1)).astype(jnp.bfloat16)


def pack_kernel(target_ref, routed_ref, rows_ref, *, experts, capacity):
    pairs, width = routed_ref.shape
    half = width // 2
    target = target_ref[...]
    named = lax.broadcasted_iota(jnp.int32, (experts, pairs), 0) == target
    earlier = jnp.dot(
        named.astype(jnp.bfloat16), strictly_before(pairs), preferred_element_type=jnp.float32
    )
    rank = jnp.sum(jnp.where(named, earlier, 0.0), axis=0, keepdims=True).astype(jnp.int32)
    slot = target * capacity + rank
    gate = routed_ref[:, :half].astype(jnp.float32)
    upper = routed_ref[:, half:].astype(jnp.float32)
    hidden = (gate / (1.0 + jnp.exp(-gate)) * upper).astype(jnp.bfloat16)
    pick = (
        lax.broadcasted_iota(jnp.int32, (experts * capacity, pairs), 0) == slot
    ).astype(jnp.bfloat16)
    rows_ref[...] = jnp.dot(pick, hidden, preferred_element_type=jnp.float32).astype(jnp.bfloat16)


def table_kernel(place_ref, routes_ref, token_ref, gate_ref, *, capacity, chosen):
    pairs = routes_ref.shape[1] // 2
    target = routes_ref[:, :pairs]
    gates = routes_ref[:, pairs:]
    before = strictly_before(pairs)
    number = (lax.broadcasted_iota(jnp.int32, target.shape, 1) // chosen).astype(jnp.float32)
    lane = lax.broadcasted_iota(jnp.int32, token_ref.shape, 1)
    period = 2 * capacity
    token = jnp.zeros(token_ref.shape, jnp.float32)
    gate = jnp.zeros(token_ref.shape, jnp.float32)
    own = place_ref[2]
    for side in range(2):
        expert = own + side * (1 - 2 * lax.rem(own, 2))
        named = target == expert.astype(jnp.float32)
        rank = jnp.dot(named.astype(jnp.bfloat16), before, preferred_element_type=jnp.float32)
        for k in range(capacity):
            found = jnp.where(named & (rank == k), 1.0, 0.0)
            here = lane % period == side * capacity + k
            token = jnp.where(here, jnp.sum(found * number, axis=1, keepdims=True), token)
            gate = jnp.where(here, jnp.sum(found * gates, axis=1, keepdims=True), gate)
    high = gate.astype(jnp.bfloat16).astype(jnp.float32)
    rest = gate - high
    middle = rest.astype(jnp.bfloat16).astype(jnp.float32)
    token_ref[...] = token
    gate_ref[...] = jnp.where(
        lane < period, high, jnp.where(lane < 2 * period, middle, rest - middle)
    )


def expert_kernel(place_ref, *refs, count):
    own_rows, other_rows = refs[:count], refs[count : 2 * count]
    own_weight, other_weight, token_ref, gate_ref, out_ref = refs[2 * count :]
    capacity = own_rows[0].shape[1]
    tokens = out_ref.shape[1]

    def project(blocks, weight):
        rows = jnp.concatenate([b[0] for b in blocks], axis=0)
        return jnp.dot(rows, weight[...], preferred_element_type=jnp.float32).astype(jnp.bfloat16)

    own = project(own_rows, own_weight)
    other = project(other_rows, other_weight)
    lanes = 6 * capacity
    wanted = lax.broadcasted_iota(jnp.int32, (tokens, lanes), 0).astype(jnp.float32)
    for i in range(count):
        at = slice(i * capacity, (i + 1) * capacity)
        stacked = jnp.concatenate([own[at], other[at]] * 3, axis=0)
        scale = jnp.where(
            token_ref[i : i + 1, :lanes] == wanted, gate_ref[i : i + 1, :lanes], 0.0
        ).astype(jnp.bfloat16)
        out_ref[i] = jnp.dot(scale, stacked, preferred_element_type=jnp.float32).astype(
            jnp.bfloat16
        )


def expert_call(place, rows, own_weight, other_weight, token, gate, homes, tokens):
    chips, both, width = rows.shape
    capacity = both // 2
    columns = own_weight.shape[1]
    piece = columns // 4
    count = len(homes)

    def row_spec(home, side):
        return pl.BlockSpec(
            (1, capacity, width),
            lambda j, s: (lax.rem(s[0] + (home + chips), chips), lax.rem(s[1] + side, 2), 0),
        )

    weight_spec = pl.BlockSpec((width, piece), lambda j, s: (0, j))
    table_spec = pl.BlockSpec(token.shape, lambda j, s: (0, 0))
    grid_spec = pltpu.PrefetchScalarGridSpec(
        num_scalar_prefetch=1,
        grid=(columns // piece,),
        in_specs=[row_spec(h, 0) for h in homes]
        + [row_spec(h, 1) for h in homes]
        + [weight_spec] * 2
        + [table_spec] * 2,
        out_specs=pl.BlockSpec((count, tokens, piece), lambda j, s: (0, 0, j)),
    )
    return pl.pallas_call(
        lambda *refs: expert_kernel(*refs, count=count),
        grid_spec=grid_spec,
        out_shape=jax.ShapeDtypeStruct((count, tokens, columns), jnp.bfloat16),
        compiler_params=pltpu.CompilerParams(
            dimension_semantics=("arbitrary",), vmem_limit_bytes=32 * 1024 * 1024
        ),
        interpret=INTERPRET,
    )(place, *([rows] * (2 * count)), own_weight, other_weight, token, gate)


def add_kernel(left_ref, right_ref, out_ref):
    def some(i, carry):
        at = pl.ds(pl.multiple_of(i * 16, 16), 16)
        total = left_ref[at].astype(jnp.float32) + right_ref[0, at].astype(jnp.float32)
        out_ref[at] = total.astype(jnp.bfloat16)
        return carry

    lax.fori_loop(0, out_ref.shape[0] // 16, some, 0)


def add_own(arrived, batch, place, chain):
    return pl.pallas_call(
        add_kernel,
        grid=(1,),
        in_specs=[
            pl.BlockSpec(arrived.shape, lambda i: (0, 0)),
            pl.BlockSpec((1,) + arrived.shape, lambda i: (place, chain, 0)),
        ],
        out_specs=pl.BlockSpec(arrived.shape, lambda i: (0, 0)),
        out_shape=jax.ShapeDtypeStruct(arrived.shape, jnp.bfloat16),
        compiler_params=pltpu.CompilerParams(vmem_limit_bytes=4 * 1024 * 1024),
        interpret=INTERPRET,
    )(arrived, batch)


def on_device(expert_ids, route_gates, routed_in, down_weight, slot_offset):
    experts = lax.axis_size("ep")
    chips = experts // 2
    tokens, chosen = expert_ids.shape
    pairs = tokens * chosen
    capacity = 2 * pairs // experts
    hidden_width = routed_in.shape[2] // 2
    weight = down_weight[0]
    index = lax.axis_index("ep")
    place = jnp.stack([index // 2, lax.rem(index, 2), index]).astype(jnp.int32)

    def shifted(value, distance):
        return lax.ppermute(
            value, "ep", [(i, (i + 2 * distance) % experts) for i in range(experts)]
        )

    target = jnp.mod(expert_ids - slot_offset[0], experts).reshape(1, pairs)
    rows = pl.pallas_call(
        lambda *refs: pack_kernel(*refs, experts=experts, capacity=capacity),
        out_shape=jax.ShapeDtypeStruct((experts * capacity, hidden_width), jnp.bfloat16),
        compiler_params=pltpu.CompilerParams(vmem_limit_bytes=32 * 1024 * 1024),
        interpret=INTERPRET,
    )(target, routed_in.reshape(pairs, 2 * hidden_width))
    same_core = [[2 * z + c for z in range(chips)] for c in range(2)]
    rows = lax.all_to_all(
        rows.reshape(chips, 2 * capacity, hidden_width),
        "ep",
        split_axis=0,
        concat_axis=0,
        axis_index_groups=same_core,
        tiled=True,
    )
    routes = jnp.concatenate([target.astype(jnp.float32), route_gates.reshape(1, pairs)], axis=1)
    origin = [0]
    distance, sign = chips // 2, 1
    while distance:
        routes = jnp.concatenate([routes, shifted(routes, sign * distance)], axis=0)
        origin = origin + [o - sign * distance for o in origin]
        distance, sign = distance // 2, -sign
    other_weight = lax.ppermute(weight, "ep", [(i, i ^ 1) for i in range(experts)])

    half = chips // 2
    batches = []
    for first in range(0, half, BATCH):
        steps = range(first, first + BATCH)
        batches.append([half - s for s in steps] + [s + 1 - half for s in steps])
    order = [origin.index(next(o for o in origin if (o - h) % chips == 0)) for b in batches for h in b]
    routes = jnp.concatenate([routes[o : o + 1] for o in order], axis=0)
    table = jax.ShapeDtypeStruct((chips, 8 * capacity), jnp.float32)
    token, gate = pl.pallas_call(
        lambda *refs: table_kernel(*refs, capacity=capacity, chosen=chosen),
        in_specs=[
            pl.BlockSpec(memory_space=pltpu.SMEM),
            pl.BlockSpec(memory_space=pltpu.VMEM),
        ],
        out_shape=(table, table),
        compiler_params=pltpu.CompilerParams(vmem_limit_bytes=8 * 1024 * 1024),
        interpret=INTERPRET,
    )(place, routes)

    sums = {}
    for n, homes in enumerate(batches):
        part = slice(n * 2 * BATCH, (n + 1) * 2 * BATCH)
        out = expert_call(
            place, rows, weight, other_weight, token[part], gate[part], homes, tokens
        )
        for i, home in enumerate(homes):
            sums[home] = (out, i)
    share = tokens // CHAINS

    def own_sum(home, c):
        batch, i = sums[home]
        return batch[i, c * share : (c + 1) * share]

    def with_own(arrived, home, c):
        batch, i = sums[home]
        return add_own(arrived, batch, i, c)

    ahead = [own_sum(half, c) for c in range(CHAINS)]
    behind = [own_sum(1 - half, c) for c in range(CHAINS)]
    for step in range(half):
        for c in range(CHAINS):
            ahead[c] = shifted(ahead[c], 1)
            if step < half - 1:
                behind[c] = shifted(behind[c], -1)
                ahead[c] = with_own(ahead[c], half - 1 - step, c)
            if step < half - 2:
                behind[c] = with_own(behind[c], step + 2 - half, c)
    return jnp.concatenate(
        [
            (
                ahead[c].astype(jnp.float32)
                + behind[c].astype(jnp.float32)
                + own_sum(0, c).astype(jnp.float32)
            ).astype(jnp.bfloat16)
            for c in range(CHAINS)
        ],
        axis=0,
    )


def solution(mesh):
    placed = (
        P(("grp", "ep"), None),
        P(("grp", "ep"), None),
        P(("grp", "ep"), None, None),
        P("ep", None, None),
        P(),
    )
    return jax.shard_map(
        on_device, mesh=mesh, in_specs=placed, out_specs=P(("grp", "ep"), None), check_vma=False
    )
```

```python
import jax
import jax.numpy as jnp
from jax import lax
from jax.experimental import pallas as pl
from jax.experimental.pallas import tpu as pltpu
from jax.sharding import PartitionSpec as P

CHAINS = 2
BATCH = 4
INTERPRET = False


def strictly_before(size):
    earlier = lax.broadcasted_iota(jnp.int32, (size, size), 0)
    return (earlier < lax.broadcasted_iota(jnp.int32, (size, size), 1)).astype(jnp.bfloat16)


def pack_kernel(
    target_ref, gate_ref, routed_ref, out_ref, hidden_ref, slot_ref, table_ref, *, capacity, chosen, blocks
):
    step = pl.program_id(0)
    pairs = target_ref.shape[1]
    chips = table_ref.shape[0]
    rows, width = routed_ref.shape
    half = width // 2
    block = out_ref.shape[0]

    @pl.when(step == 0)
    def _():
        target = target_ref[...]
        named = lax.broadcasted_iota(jnp.int32, (2 * chips, pairs), 0) == target
        earlier = jnp.dot(
            named.astype(jnp.bfloat16), strictly_before(pairs), preferred_element_type=jnp.float32
        )
        rank = jnp.sum(jnp.where(named, earlier, 0.0), axis=0, keepdims=True).astype(jnp.int32)
        slot_ref[...] = target * capacity + rank
        at_rank = (lax.broadcasted_iota(jnp.int32, (capacity, pairs), 0) == rank).astype(jnp.bfloat16)
        token = (lax.broadcasted_iota(jnp.int32, (1, pairs), 1) // chosen).astype(jnp.float32)
        gate = gate_ref[...]
        high = gate.astype(jnp.bfloat16).astype(jnp.float32)
        rest = gate - high
        middle = rest.astype(jnp.bfloat16).astype(jnp.float32)
        table_ref[...] = jnp.zeros(table_ref.shape, jnp.float32)
        for side in range(2):
            mine = 2 * lax.broadcasted_iota(jnp.int32, (chips, pairs), 0) + side == target
            for kind, value in enumerate((token, high, middle, rest - middle)):
                found = lax.dot_general(
                    jnp.where(mine, value, 0.0).astype(jnp.bfloat16),
                    at_rank,
                    (((1,), (1,)), ((), ())),
                    preferred_element_type=jnp.float32,
                )
                for copy in range(3) if kind == 0 else (kind - 1,):
                    start = (2 * copy + side) * capacity
                    table_ref[:, min(kind, 1), start : start + capacity] = found

    @pl.when(step < blocks)
    def _():
        gate = routed_ref[:, :half].astype(jnp.float32)
        upper = routed_ref[:, half:].astype(jnp.float32)
        hidden = (gate / (1.0 + jnp.exp(-gate)) * upper).astype(jnp.bfloat16)
        hidden_ref[pl.ds(pl.multiple_of(step * rows, rows), rows), :] = hidden

    @pl.when(step >= blocks)
    def _():
        first = (step - blocks) * block
        slots = block * 2 * capacity
        wanted = lax.broadcasted_iota(jnp.int32, (slots, pairs), 0) + first * 2 * capacity
        pick = (wanted == slot_ref[...]).astype(jnp.bfloat16)
        chosen_rows = jnp.dot(pick, hidden_ref[...], preferred_element_type=jnp.float32).astype(
            jnp.bfloat16
        )
        for chip in range(block):
            for tile in range(half // 128):
                out_ref[chip, tile * 2 * capacity : (tile + 1) * 2 * capacity, :] = chosen_rows[
                    chip * 2 * capacity : (chip + 1) * 2 * capacity, tile * 128 : (tile + 1) * 128
                ]
        out_ref[:, (half // 128) * 2 * capacity :, :] = table_ref[
            pl.ds(pl.multiple_of(first, block), block)
        ].astype(jnp.bfloat16)


def pack(target, gates, routed, chips, capacity, chosen):
    pairs, width = routed.shape
    blocks = 4
    tall = width // 256 * 2 * capacity + 8
    return pl.pallas_call(
        lambda *refs: pack_kernel(*refs, capacity=capacity, chosen=chosen, blocks=blocks),
        grid=(2 * blocks,),
        in_specs=[
            pl.BlockSpec(target.shape, lambda i: (0, 0)),
            pl.BlockSpec(gates.shape, lambda i: (0, 0)),
            pl.BlockSpec((pairs // blocks, width), lambda i: (jnp.minimum(i, blocks - 1), 0)),
        ],
        out_specs=pl.BlockSpec(
            (chips // blocks, tall, 128), lambda i: (jnp.maximum(i - blocks, 0), 0, 0)
        ),
        out_shape=jax.ShapeDtypeStruct((chips, tall, 128), jnp.bfloat16),
        scratch_shapes=[
            pltpu.VMEM((pairs, width // 2), jnp.bfloat16),
            pltpu.VMEM((1, pairs), jnp.int32),
            pltpu.VMEM((chips, 8, 128), jnp.float32),
        ],
        compiler_params=pltpu.CompilerParams(
            dimension_semantics=("arbitrary",), vmem_limit_bytes=60 * 1024 * 1024
        ),
        interpret=INTERPRET,
    )(target, gates, routed)


def expert_kernel(place_ref, *refs, count, capacity):
    packed = refs[:count]
    own_weight, other_weight, out_ref = refs[count:]
    tokens = out_ref.shape[1]
    core = place_ref[1]
    tiles = own_weight.shape[0] // 128

    def project(side, weight):
        blocks = [
            jnp.concatenate(
                [
                    p[0, pl.ds(pl.multiple_of((2 * t + side) * capacity, capacity), capacity), :]
                    for t in range(tiles)
                ],
                axis=1,
            )
            for p in packed
        ]
        rows = jnp.concatenate(blocks, axis=0)
        return jnp.dot(rows, weight[...], preferred_element_type=jnp.float32).astype(jnp.bfloat16)

    own = project(core, own_weight)
    other = project(1 - core, other_weight)
    lower = jnp.where(core == 0, own, other)
    upper = jnp.where(core == 0, other, own)
    lanes = 6 * capacity
    wanted = lax.broadcasted_iota(jnp.int32, (tokens, lanes), 0).astype(jnp.float32)
    for i, p in enumerate(packed):
        at = slice(i * capacity, (i + 1) * capacity)
        stacked = jnp.concatenate([lower[at], upper[at]] * 3, axis=0)
        table = p[0, tiles * 2 * capacity :, :].astype(jnp.float32)
        scale = jnp.where(table[0:1, :lanes] == wanted, table[1:2, :lanes], 0.0).astype(jnp.bfloat16)
        out_ref[i] = jnp.dot(scale, stacked, preferred_element_type=jnp.float32).astype(
            jnp.bfloat16
        )


def expert_call(place, packed, own_weight, other_weight, homes, tokens, capacity, chain):
    chips, tall, _ = packed.shape
    width, columns = own_weight.shape
    columns = columns // CHAINS
    steps = 2
    piece = columns // steps
    count = len(homes)

    def row_spec(home):
        return pl.BlockSpec(
            (1, tall, 128), lambda j, s: (lax.rem(s[0] + (home + chips), chips), 0, 0)
        )

    weight_spec = pl.BlockSpec((width, piece), lambda j, s: (0, chain * steps + j))
    grid_spec = pltpu.PrefetchScalarGridSpec(
        num_scalar_prefetch=1,
        grid=(steps,),
        in_specs=[row_spec(h) for h in homes] + [weight_spec] * 2,
        out_specs=pl.BlockSpec((count, tokens, piece), lambda j, s: (0, 0, j)),
    )
    flops = 4 * count * capacity * width * columns
    return pl.pallas_call(
        lambda *refs: expert_kernel(*refs, count=count, capacity=capacity),
        grid_spec=grid_spec,
        out_shape=jax.ShapeDtypeStruct((count, tokens, columns), jnp.bfloat16),
        cost_estimate=pl.CostEstimate(
            flops=flops, bytes_accessed=4 * width * columns, transcendentals=0
        ),
        compiler_params=pltpu.CompilerParams(
            dimension_semantics=("arbitrary",), vmem_limit_bytes=48 * 1024 * 1024
        ),
        interpret=INTERPRET,
    )(place, *([packed] * count), own_weight, other_weight)


def add_kernel(left_ref, right_ref, out_ref):
    def some(i, carry):
        at = pl.ds(pl.multiple_of(i * 16, 16), 16)
        total = left_ref[at].astype(jnp.float32) + right_ref[0, at].astype(jnp.float32)
        out_ref[at] = total.astype(jnp.bfloat16)
        return carry

    lax.fori_loop(0, out_ref.shape[0] // 16, some, 0)


def add_own(arrived, batch, place):
    return pl.pallas_call(
        add_kernel,
        grid=(1,),
        in_specs=[
            pl.BlockSpec(arrived.shape, lambda i: (0, 0)),
            pl.BlockSpec((1,) + arrived.shape, lambda i: (place, 0, 0)),
        ],
        out_specs=pl.BlockSpec(arrived.shape, lambda i: (0, 0)),
        out_shape=jax.ShapeDtypeStruct(arrived.shape, jnp.bfloat16),
        compiler_params=pltpu.CompilerParams(vmem_limit_bytes=4 * 1024 * 1024),
        interpret=INTERPRET,
    )(arrived, batch)


def on_device(expert_ids, route_gates, routed_in, down_weight, slot_offset):
    experts = lax.axis_size("ep")
    chips = experts // 2
    tokens, chosen = expert_ids.shape
    pairs = tokens * chosen
    capacity = 2 * pairs // experts
    weight = down_weight[0]
    index = lax.axis_index("ep")
    place = jnp.stack([index // 2, lax.rem(index, 2)]).astype(jnp.int32)

    def shifted(value, distance):
        return lax.ppermute(
            value, "ep", [(i, (i + 2 * distance) % experts) for i in range(experts)]
        )

    target = jnp.mod(expert_ids - slot_offset[0], experts).reshape(1, pairs)
    packed = pack(
        target,
        route_gates.reshape(1, pairs),
        routed_in.reshape(pairs, routed_in.shape[2]),
        chips,
        capacity,
        chosen,
    )
    same_core = [[2 * z + c for z in range(chips)] for c in range(2)]
    other_weight = lax.ppermute(weight, "ep", [(i, i ^ 1) for i in range(experts)])
    packed = lax.all_to_all(
        packed,
        "ep",
        split_axis=0,
        concat_axis=0,
        axis_index_groups=same_core,
        tiled=True,
    )

    half = chips // 2
    sums = {}
    for first in range(0, half, BATCH):
        steps = range(first, first + BATCH)
        homes = [half - s for s in steps] + [s + 1 - half for s in steps]
        for c in range(CHAINS):
            out = expert_call(place, packed, weight, other_weight, homes, tokens, capacity, c)
            for i, home in enumerate(homes):
                sums[home, c] = (out, i)

    def own_sum(home, c):
        batch, i = sums[home, c]
        return batch[i]

    def with_own(arrived, home, c):
        return add_own(arrived, *sums[home, c])

    ahead = [own_sum(half, c) for c in range(CHAINS)]
    behind = [own_sum(1 - half, c) for c in range(CHAINS)]
    for step in range(half):
        for c in range(CHAINS):
            ahead[c] = shifted(ahead[c], 1)
            if step < half - 1:
                behind[c] = shifted(behind[c], -1)
                ahead[c] = with_own(ahead[c], half - 1 - step, c)
            if step < half - 2:
                behind[c] = with_own(behind[c], step + 2 - half, c)
    return jnp.concatenate(
        [
            (
                ahead[c].astype(jnp.float32)
                + behind[c].astype(jnp.float32)
                + own_sum(0, c).astype(jnp.float32)
            ).astype(jnp.bfloat16)
            for c in range(CHAINS)
        ],
        axis=1,
    )


def solution(mesh):
    placed = (
        P(("grp", "ep"), None),
        P(("grp", "ep"), None),
        P(("grp", "ep"), None, None),
        P("ep", None, None),
        P(),
    )
    return jax.shard_map(
        on_device, mesh=mesh, in_specs=placed, out_specs=P(("grp", "ep"), None), check_vma=False
    )
```

```python
import jax
import jax.numpy as jnp
from jax import lax
from jax.experimental import pallas as pl
from jax.experimental.pallas import tpu as pltpu
from jax.sharding import PartitionSpec as P

CHAINS = 2
STEPS = (4, 6, 6)
PIECES = (1, 2, 2)
PARTS = 4
INTERPRET = False


def strictly_before(size):
    earlier = lax.broadcasted_iota(jnp.int32, (size, size), 0)
    return (earlier < lax.broadcasted_iota(jnp.int32, (size, size), 1)).astype(jnp.bfloat16)


def pack_kernel(
    target_ref,
    gate_ref,
    routed_ref,
    out_ref,
    raw_ref,
    hidden_ref,
    table_ref,
    packed_ref,
    arrive,
    leave,
    *,
    capacity,
    chosen,
):
    pairs = target_ref.shape[1]
    chips = table_ref.shape[0]
    half = routed_ref.shape[1] // 2
    rows = pairs // PARTS
    block = chips // PARTS
    reads = [
        pltpu.make_async_copy(
            routed_ref.at[pl.ds(i * rows, rows)], raw_ref.at[pl.ds(i * rows, rows)], arrive.at[i]
        )
        for i in range(PARTS)
    ]
    writes = [
        pltpu.make_async_copy(
            packed_ref.at[pl.ds(i * block, block)], out_ref.at[pl.ds(i * block, block)], leave.at[i]
        )
        for i in range(PARTS)
    ]
    for read in reads:
        read.start()
    target = target_ref[...]
    named = lax.broadcasted_iota(jnp.int32, (2 * chips, pairs), 0) == target
    earlier = jnp.dot(
        named.astype(jnp.bfloat16), strictly_before(pairs), preferred_element_type=jnp.float32
    )
    rank = jnp.sum(jnp.where(named, earlier, 0.0), axis=0, keepdims=True).astype(jnp.int32)
    slot = target * capacity + rank
    at_rank = (lax.broadcasted_iota(jnp.int32, (capacity, pairs), 0) == rank).astype(jnp.bfloat16)
    token = (lax.broadcasted_iota(jnp.int32, (1, pairs), 1) // chosen).astype(jnp.float32)
    gate = gate_ref[...]
    high = gate.astype(jnp.bfloat16).astype(jnp.float32)
    rest = gate - high
    middle = rest.astype(jnp.bfloat16).astype(jnp.float32)
    table_ref[...] = jnp.zeros(table_ref.shape, jnp.float32)
    for side in range(2):
        mine = 2 * lax.broadcasted_iota(jnp.int32, (chips, pairs), 0) + side == target
        for kind, value in enumerate((token, high, middle, rest - middle)):
            found = lax.dot_general(
                jnp.where(mine, value, 0.0).astype(jnp.bfloat16),
                at_rank,
                (((1,), (1,)), ((), ())),
                preferred_element_type=jnp.float32,
            )
            for copy in range(3) if kind == 0 else (kind - 1,):
                start = (2 * copy + side) * capacity
                table_ref[:, min(kind, 1), start : start + capacity] = found
    for i, read in enumerate(reads):
        read.wait()
        at = slice(i * rows, (i + 1) * rows)
        gate = raw_ref[at, :half].astype(jnp.float32)
        upper = raw_ref[at, half:].astype(jnp.float32)
        hidden_ref[at, :] = (gate / (1.0 + jnp.exp(-gate)) * upper).astype(jnp.bfloat16)
    slots = block * 2 * capacity
    for i, write in enumerate(writes):
        wanted = lax.broadcasted_iota(jnp.int32, (slots, pairs), 0) + i * slots
        picked = jnp.dot(
            (wanted == slot).astype(jnp.bfloat16),
            hidden_ref[...],
            preferred_element_type=jnp.float32,
        ).astype(jnp.bfloat16)
        for chip in range(block):
            for tile in range(half // 128):
                packed_ref[i * block + chip, tile * 2 * capacity : (tile + 1) * 2 * capacity, :] = (
                    picked[
                        chip * 2 * capacity : (chip + 1) * 2 * capacity,
                        tile * 128 : (tile + 1) * 128,
                    ]
                )
        packed_ref[i * block : (i + 1) * block, (half // 128) * 2 * capacity :, :] = table_ref[
            i * block : (i + 1) * block
        ].astype(jnp.bfloat16)
        write.start()
    for write in writes:
        write.wait()


def pack(target, gates, routed, chips, capacity, chosen):
    pairs, width = routed.shape
    tall = width // 256 * 2 * capacity + 8
    return pl.pallas_call(
        lambda *refs: pack_kernel(*refs, capacity=capacity, chosen=chosen),
        in_specs=[
            pl.BlockSpec(memory_space=pltpu.VMEM),
            pl.BlockSpec(memory_space=pltpu.VMEM),
            pl.BlockSpec(memory_space=pltpu.HBM),
        ],
        out_specs=pl.BlockSpec(memory_space=pltpu.HBM),
        out_shape=jax.ShapeDtypeStruct((chips, tall, 128), jnp.bfloat16),
        scratch_shapes=[
            pltpu.VMEM((pairs, width), jnp.bfloat16),
            pltpu.VMEM((pairs, width // 2), jnp.bfloat16),
            pltpu.VMEM((chips, 8, 128), jnp.float32),
            pltpu.VMEM((chips, tall, 128), jnp.bfloat16),
            pltpu.SemaphoreType.DMA((PARTS,)),
            pltpu.SemaphoreType.DMA((PARTS,)),
        ],
        compiler_params=pltpu.CompilerParams(vmem_limit_bytes=60 * 1024 * 1024),
        interpret=INTERPRET,
    )(target, gates, routed)


def expert_kernel(place_ref, *refs, count, capacity):
    packed = refs[:count]
    own_weight, other_weight, out_ref = refs[count:]
    tokens = out_ref.shape[1]
    core = place_ref[1]
    tiles = own_weight.shape[0] // 128

    def project(side, weight):
        blocks = [
            jnp.concatenate(
                [
                    p[0, pl.ds(pl.multiple_of((2 * t + side) * capacity, capacity), capacity), :]
                    for t in range(tiles)
                ],
                axis=1,
            )
            for p in packed
        ]
        rows = jnp.concatenate(blocks, axis=0)
        return jnp.dot(rows, weight[...], preferred_element_type=jnp.float32).astype(jnp.bfloat16)

    own = project(core, own_weight)
    other = project(1 - core, other_weight)
    lower = jnp.where(core == 0, own, other)
    upper = jnp.where(core == 0, other, own)
    lanes = 6 * capacity
    wanted = lax.broadcasted_iota(jnp.int32, (tokens, lanes), 0).astype(jnp.float32)
    for i, p in enumerate(packed):
        at = slice(i * capacity, (i + 1) * capacity)
        stacked = jnp.concatenate([lower[at], upper[at]] * 3, axis=0)
        table = p[0, tiles * 2 * capacity :, :].astype(jnp.float32)
        scale = jnp.where(table[0:1, :lanes] == wanted, table[1:2, :lanes], 0.0).astype(jnp.bfloat16)
        out_ref[i] = jnp.dot(scale, stacked, preferred_element_type=jnp.float32).astype(
            jnp.bfloat16
        )


def expert_call(place, packed, own_weight, other_weight, homes, tokens, capacity, part, parts):
    chips, tall, _ = packed.shape
    width, columns = own_weight.shape
    columns = columns // parts
    steps = 2 if parts == CHAINS else 1
    piece = columns // steps
    count = len(homes)

    def row_spec(home):
        return pl.BlockSpec(
            (1, tall, 128), lambda j, s: (lax.rem(s[0] + (home + chips), chips), 0, 0)
        )

    weight_spec = pl.BlockSpec((width, piece), lambda j, s: (0, part * steps + j))
    grid_spec = pltpu.PrefetchScalarGridSpec(
        num_scalar_prefetch=1,
        grid=(steps,),
        in_specs=[row_spec(h) for h in homes] + [weight_spec] * 2,
        out_specs=pl.BlockSpec((count, tokens, piece), lambda j, s: (0, 0, j)),
    )
    flops = 4 * count * capacity * width * columns
    return pl.pallas_call(
        lambda *refs: expert_kernel(*refs, count=count, capacity=capacity),
        grid_spec=grid_spec,
        out_shape=jax.ShapeDtypeStruct((count, tokens, columns), jnp.bfloat16),
        cost_estimate=pl.CostEstimate(
            flops=flops, bytes_accessed=4 * width * columns, transcendentals=0
        ),
        compiler_params=pltpu.CompilerParams(
            dimension_semantics=("arbitrary",), vmem_limit_bytes=48 * 1024 * 1024
        ),
        interpret=INTERPRET,
    )(place, *([packed] * count), own_weight, other_weight)


def add_kernel(left_ref, *refs):
    own, out_ref = refs[:-1], refs[-1]
    wide = out_ref.shape[1] // len(own)

    def some(i, carry):
        at = pl.ds(pl.multiple_of(i * 16, 16), 16)
        for n, right_ref in enumerate(own):
            to = slice(n * wide, (n + 1) * wide)
            total = left_ref[at, to].astype(jnp.float32) + right_ref[0, at].astype(jnp.float32)
            out_ref[at, to] = total.astype(jnp.bfloat16)
        return carry

    lax.fori_loop(0, out_ref.shape[0] // 16, some, 0)


def add_own(arrived, batches, place):
    whole = pl.BlockSpec(arrived.shape, lambda i: (0, 0))
    return pl.pallas_call(
        add_kernel,
        grid=(1,),
        in_specs=[whole]
        + [pl.BlockSpec((1,) + batch.shape[1:], lambda i: (place, 0, 0)) for batch in batches],
        out_specs=whole,
        out_shape=jax.ShapeDtypeStruct(arrived.shape, jnp.bfloat16),
        compiler_params=pltpu.CompilerParams(vmem_limit_bytes=4 * 1024 * 1024),
        interpret=INTERPRET,
    )(arrived, *batches)


def on_device(expert_ids, route_gates, routed_in, down_weight, slot_offset):
    experts = lax.axis_size("ep")
    chips = experts // 2
    tokens, chosen = expert_ids.shape
    pairs = tokens * chosen
    capacity = 2 * pairs // experts
    weight = down_weight[0]
    index = lax.axis_index("ep")
    place = jnp.stack([index // 2, lax.rem(index, 2)]).astype(jnp.int32)

    def shifted(value, distance):
        return lax.ppermute(
            value, "ep", [(i, (i + 2 * distance) % experts) for i in range(experts)]
        )

    target = jnp.mod(expert_ids - slot_offset[0], experts).reshape(1, pairs)
    packed = pack(
        target,
        route_gates.reshape(1, pairs),
        routed_in.reshape(pairs, routed_in.shape[2]),
        chips,
        capacity,
        chosen,
    )
    same_core = [[2 * z + c for z in range(chips)] for c in range(2)]
    other_weight = lax.ppermute(weight, "ep", [(i, i ^ 1) for i in range(experts)])
    packed = lax.all_to_all(
        packed,
        "ep",
        split_axis=0,
        concat_axis=0,
        axis_index_groups=same_core,
        tiled=True,
    )


    half = chips // 2
    sums = {}
    first = 0
    for count, pieces in zip(STEPS, PIECES):
        steps = range(first, first + count)
        first += count
        homes = [half - s for s in steps] + [s + 1 - half for s in steps]
        for c in range(CHAINS):
            batches = []
            for piece in range(pieces):
                batches.append(
                    expert_call(
                        place,
                        packed,
                        weight,
                        other_weight,
                        homes,
                        tokens,
                        capacity,
                        c * pieces + piece,
                        CHAINS * pieces,
                    )
                )
            for i, home in enumerate(homes):
                sums[home, c] = (batches, i)

    def own_sum(home, c):
        batches, i = sums[home, c]
        return jnp.concatenate([batch[i] for batch in batches], axis=1)

    def with_own(arrived, home, c):
        return add_own(arrived, *sums[home, c])

    ahead = [own_sum(half, c) for c in range(CHAINS)]
    behind = [own_sum(1 - half, c) for c in range(CHAINS)]
    for step in range(half):
        for c in range(CHAINS):
            ahead[c] = shifted(ahead[c], 1)
            if step < half - 1:
                behind[c] = shifted(behind[c], -1)
                ahead[c] = with_own(ahead[c], half - 1 - step, c)
            if step < half - 2:
                behind[c] = with_own(behind[c], step + 2 - half, c)
    return jnp.concatenate(
        [
            (
                ahead[c].astype(jnp.float32)
                + behind[c].astype(jnp.float32)
                + own_sum(0, c).astype(jnp.float32)
            ).astype(jnp.bfloat16)
            for c in range(CHAINS)
        ],
        axis=1,
    )


def solution(mesh):
    placed = (
        P(("grp", "ep"), None),
        P(("grp", "ep"), None),
        P(("grp", "ep"), None, None),
        P("ep", None, None),
        P(),
    )
    return jax.shard_map(
        on_device, mesh=mesh, in_specs=placed, out_specs=P(("grp", "ep"), None), check_vma=False
    )
```

```python
import jax
import jax.numpy as jnp
from jax import lax
from jax.experimental import pallas as pl
from jax.experimental.pallas import tpu as pltpu
from jax.sharding import PartitionSpec as P

CHAINS = 2
STEPS = (4, 4, 4, 4)
PIECES = (1, 2, 2, 2)
PARTS = 4
INTERPRET = False


def strictly_before(size):
    earlier = lax.broadcasted_iota(jnp.int32, (size, size), 0)
    return (earlier < lax.broadcasted_iota(jnp.int32, (size, size), 1)).astype(jnp.bfloat16)


def pack_kernel(
    target_ref,
    gate_ref,
    routed_ref,
    out_ref,
    raw_ref,
    hidden_ref,
    table_ref,
    packed_ref,
    arrive,
    leave,
    *,
    capacity,
    chosen,
):
    pairs = target_ref.shape[1]
    chips = table_ref.shape[0]
    half = routed_ref.shape[1] // 2
    rows = pairs // PARTS
    block = chips // PARTS
    reads = [
        pltpu.make_async_copy(
            routed_ref.at[pl.ds(i * rows, rows)], raw_ref.at[pl.ds(i * rows, rows)], arrive.at[i]
        )
        for i in range(PARTS)
    ]
    writes = [
        pltpu.make_async_copy(
            packed_ref.at[pl.ds(i * block, block)], out_ref.at[pl.ds(i * block, block)], leave.at[i]
        )
        for i in range(PARTS)
    ]
    for read in reads:
        read.start()
    target = target_ref[...]
    named = lax.broadcasted_iota(jnp.int32, (2 * chips, pairs), 0) == target
    earlier = jnp.dot(
        named.astype(jnp.bfloat16), strictly_before(pairs), preferred_element_type=jnp.float32
    )
    rank = jnp.sum(jnp.where(named, earlier, 0.0), axis=0, keepdims=True).astype(jnp.int32)
    slot = target * capacity + rank
    at_rank = (lax.broadcasted_iota(jnp.int32, (capacity, pairs), 0) == rank).astype(jnp.bfloat16)
    token = (lax.broadcasted_iota(jnp.int32, (1, pairs), 1) // chosen).astype(jnp.float32)
    gate = gate_ref[...]
    high = gate.astype(jnp.bfloat16).astype(jnp.float32)
    rest = gate - high
    middle = rest.astype(jnp.bfloat16).astype(jnp.float32)
    table_ref[...] = jnp.zeros(table_ref.shape, jnp.float32)
    for side in range(2):
        mine = 2 * lax.broadcasted_iota(jnp.int32, (chips, pairs), 0) + side == target
        for kind, value in enumerate((token, high, middle, rest - middle)):
            found = lax.dot_general(
                jnp.where(mine, value, 0.0).astype(jnp.bfloat16),
                at_rank,
                (((1,), (1,)), ((), ())),
                preferred_element_type=jnp.float32,
            )
            for copy in range(3) if kind == 0 else (kind - 1,):
                start = (2 * copy + side) * capacity
                table_ref[:, min(kind, 1), start : start + capacity] = found
    for i, read in enumerate(reads):
        read.wait()
        at = slice(i * rows, (i + 1) * rows)
        gate = raw_ref[at, :half].astype(jnp.float32)
        upper = raw_ref[at, half:].astype(jnp.float32)
        hidden_ref[at, :] = (gate / (1.0 + jnp.exp(-gate)) * upper).astype(jnp.bfloat16)
    slots = block * 2 * capacity
    for i, write in enumerate(writes):
        wanted = lax.broadcasted_iota(jnp.int32, (slots, pairs), 0) + i * slots
        picked = jnp.dot(
            (wanted == slot).astype(jnp.bfloat16),
            hidden_ref[...],
            preferred_element_type=jnp.float32,
        ).astype(jnp.bfloat16)
        for chip in range(block):
            for tile in range(half // 128):
                packed_ref[i * block + chip, tile * 2 * capacity : (tile + 1) * 2 * capacity, :] = (
                    picked[
                        chip * 2 * capacity : (chip + 1) * 2 * capacity,
                        tile * 128 : (tile + 1) * 128,
                    ]
                )
        packed_ref[i * block : (i + 1) * block, (half // 128) * 2 * capacity :, :] = table_ref[
            i * block : (i + 1) * block
        ].astype(jnp.bfloat16)
        write.start()
    for write in writes:
        write.wait()


def pack(target, gates, routed, chips, capacity, chosen):
    pairs, width = routed.shape
    tall = width // 256 * 2 * capacity + 8
    return pl.pallas_call(
        lambda *refs: pack_kernel(*refs, capacity=capacity, chosen=chosen),
        in_specs=[
            pl.BlockSpec(memory_space=pltpu.VMEM),
            pl.BlockSpec(memory_space=pltpu.VMEM),
            pl.BlockSpec(memory_space=pltpu.HBM),
        ],
        out_specs=pl.BlockSpec(memory_space=pltpu.HBM),
        out_shape=jax.ShapeDtypeStruct((chips, tall, 128), jnp.bfloat16),
        scratch_shapes=[
            pltpu.VMEM((pairs, width), jnp.bfloat16),
            pltpu.VMEM((pairs, width // 2), jnp.bfloat16),
            pltpu.VMEM((chips, 8, 128), jnp.float32),
            pltpu.VMEM((chips, tall, 128), jnp.bfloat16),
            pltpu.SemaphoreType.DMA((PARTS,)),
            pltpu.SemaphoreType.DMA((PARTS,)),
        ],
        compiler_params=pltpu.CompilerParams(vmem_limit_bytes=60 * 1024 * 1024),
        interpret=INTERPRET,
    )(target, gates, routed)


def expert_kernel(place_ref, *refs, count, capacity):
    packed = refs[:count]
    own_weight, other_weight, out_ref = refs[count:]
    tokens = out_ref.shape[1]
    core = place_ref[1]
    tiles = own_weight.shape[0] // 128

    def project(side, weight):
        blocks = [
            jnp.concatenate(
                [
                    p[0, pl.ds(pl.multiple_of((2 * t + side) * capacity, capacity), capacity), :]
                    for t in range(tiles)
                ],
                axis=1,
            )
            for p in packed
        ]
        rows = jnp.concatenate(blocks, axis=0)
        return jnp.dot(rows, weight[...], preferred_element_type=jnp.float32).astype(jnp.bfloat16)

    own = project(core, own_weight)
    other = project(1 - core, other_weight)
    lower = jnp.where(core == 0, own, other)
    upper = jnp.where(core == 0, other, own)
    lanes = 4 * capacity
    wanted = lax.broadcasted_iota(jnp.int32, (tokens, lanes), 0).astype(jnp.float32)
    for i, p in enumerate(packed):
        at = slice(i * capacity, (i + 1) * capacity)
        stacked = jnp.concatenate([lower[at], upper[at]] * 2, axis=0)
        table = p[0, tiles * 2 * capacity :, :].astype(jnp.float32)
        scale = jnp.where(table[0:1, :lanes] == wanted, table[1:2, :lanes], 0.0).astype(jnp.bfloat16)
        out_ref[i] = jnp.dot(scale, stacked, preferred_element_type=jnp.float32).astype(
            jnp.bfloat16
        )


def expert_call(place, packed, own_weight, other_weight, homes, tokens, capacity, part, parts):
    chips, tall, _ = packed.shape
    width, columns = own_weight.shape
    columns = columns // parts
    steps = 2 if parts == CHAINS else 1
    piece = columns // steps
    count = len(homes)

    def row_spec(home):
        return pl.BlockSpec(
            (1, tall, 128), lambda j, s: (lax.rem(s[0] + (home + chips), chips), 0, 0)
        )

    weight_spec = pl.BlockSpec((width, piece), lambda j, s: (0, part * steps + j))
    grid_spec = pltpu.PrefetchScalarGridSpec(
        num_scalar_prefetch=1,
        grid=(steps,),
        in_specs=[row_spec(h) for h in homes] + [weight_spec] * 2,
        out_specs=pl.BlockSpec((count, tokens, piece), lambda j, s: (0, 0, j)),
    )
    flops = 4 * count * capacity * width * columns
    return pl.pallas_call(
        lambda *refs: expert_kernel(*refs, count=count, capacity=capacity),
        grid_spec=grid_spec,
        out_shape=jax.ShapeDtypeStruct((count, tokens, columns), jnp.bfloat16),
        cost_estimate=pl.CostEstimate(
            flops=flops, bytes_accessed=4 * width * columns, transcendentals=0
        ),
        compiler_params=pltpu.CompilerParams(
            dimension_semantics=("arbitrary",), vmem_limit_bytes=48 * 1024 * 1024
        ),
        interpret=INTERPRET,
    )(place, *([packed] * count), own_weight, other_weight)


def add_kernel(left_ref, *refs):
    own, out_ref = refs[:-1], refs[-1]
    wide = out_ref.shape[1] // len(own)

    def some(i, carry):
        at = pl.ds(pl.multiple_of(i * 16, 16), 16)
        for n, right_ref in enumerate(own):
            to = slice(n * wide, (n + 1) * wide)
            total = left_ref[at, to].astype(jnp.float32) + right_ref[0, at].astype(jnp.float32)
            out_ref[at, to] = total.astype(jnp.bfloat16)
        return carry

    lax.fori_loop(0, out_ref.shape[0] // 16, some, 0)


def add_own(arrived, batches, place):
    whole = pl.BlockSpec(arrived.shape, lambda i: (0, 0))
    return pl.pallas_call(
        add_kernel,
        grid=(1,),
        in_specs=[whole]
        + [pl.BlockSpec((1,) + batch.shape[1:], lambda i: (place, 0, 0)) for batch in batches],
        out_specs=whole,
        out_shape=jax.ShapeDtypeStruct(arrived.shape, jnp.bfloat16),
        compiler_params=pltpu.CompilerParams(vmem_limit_bytes=4 * 1024 * 1024),
        interpret=INTERPRET,
    )(arrived, *batches)


def on_device(expert_ids, route_gates, routed_in, down_weight, slot_offset):
    experts = lax.axis_size("ep")
    chips = experts // 2
    tokens, chosen = expert_ids.shape
    pairs = tokens * chosen
    capacity = 2 * pairs // experts
    weight = down_weight[0]
    index = lax.axis_index("ep")
    place = jnp.stack([index // 2, lax.rem(index, 2)]).astype(jnp.int32)

    def shifted(value, distance):
        return lax.ppermute(
            value, "ep", [(i, (i + 2 * distance) % experts) for i in range(experts)]
        )

    target = jnp.mod(expert_ids - slot_offset[0], experts).reshape(1, pairs)
    packed = pack(
        target,
        route_gates.reshape(1, pairs),
        routed_in.reshape(pairs, routed_in.shape[2]),
        chips,
        capacity,
        chosen,
    )
    same_core = [[2 * z + c for z in range(chips)] for c in range(2)]
    other_weight = lax.ppermute(weight, "ep", [(i, i ^ 1) for i in range(experts)])
    packed = lax.all_to_all(
        packed,
        "ep",
        split_axis=0,
        concat_axis=0,
        axis_index_groups=same_core,
        tiled=True,
    )


    half = chips // 2
    sums = {}
    first = 0
    for count, pieces in zip(STEPS, PIECES):
        steps = range(first, first + count)
        first += count
        homes = [half - s for s in steps] + [s + 1 - half for s in steps]
        for c in range(CHAINS):
            batches = []
            for piece in range(pieces):
                batches.append(
                    expert_call(
                        place,
                        packed,
                        weight,
                        other_weight,
                        homes,
                        tokens,
                        capacity,
                        c * pieces + piece,
                        CHAINS * pieces,
                    )
                )
            for i, home in enumerate(homes):
                sums[home, c] = (batches, i)

    def own_sum(home, c):
        batches, i = sums[home, c]
        return jnp.concatenate([batch[i] for batch in batches], axis=1)

    def with_own(arrived, home, c):
        return add_own(arrived, *sums[home, c])

    ahead = [own_sum(half, c) for c in range(CHAINS)]
    behind = [own_sum(1 - half, c) for c in range(CHAINS)]
    for step in range(half):
        for c in range(CHAINS):
            ahead[c] = shifted(ahead[c], 1)
            if step < half - 1:
                behind[c] = shifted(behind[c], -1)
                ahead[c] = with_own(ahead[c], half - 1 - step, c)
            if step < half - 2:
                behind[c] = with_own(behind[c], step + 2 - half, c)
    return jnp.concatenate(
        [
            (
                ahead[c].astype(jnp.float32)
                + behind[c].astype(jnp.float32)
                + own_sum(0, c).astype(jnp.float32)
            ).astype(jnp.bfloat16)
            for c in range(CHAINS)
        ],
        axis=1,
    )


def solution(mesh):
    placed = (
        P(("grp", "ep"), None),
        P(("grp", "ep"), None),
        P(("grp", "ep"), None, None),
        P("ep", None, None),
        P(),
    )
    return jax.shard_map(
        on_device, mesh=mesh, in_specs=placed, out_specs=P(("grp", "ep"), None), check_vma=False
    )
```

```python
import jax
import jax.numpy as jnp
from jax import lax
from jax.experimental import pallas as pl
from jax.experimental.pallas import tpu as pltpu
from jax.sharding import PartitionSpec as P

CHAINS = 2
STEPS = (4, 4, 4, 4)
PIECES = (1, 4, 4, 4)
PARTS = 4
INTERPRET = False


def strictly_before(size):
    earlier = lax.broadcasted_iota(jnp.int32, (size, size), 0)
    return (earlier < lax.broadcasted_iota(jnp.int32, (size, size), 1)).astype(jnp.bfloat16)


def pack_kernel(
    target_ref,
    gate_ref,
    routed_ref,
    out_ref,
    raw_ref,
    hidden_ref,
    table_ref,
    packed_ref,
    arrive,
    leave,
    *,
    capacity,
    chosen,
):
    pairs = target_ref.shape[1]
    chips = table_ref.shape[0]
    half = routed_ref.shape[1] // 2
    rows = pairs // PARTS
    block = chips // PARTS
    reads = [
        pltpu.make_async_copy(
            routed_ref.at[pl.ds(i * rows, rows)], raw_ref.at[pl.ds(i * rows, rows)], arrive.at[i]
        )
        for i in range(PARTS)
    ]
    writes = [
        pltpu.make_async_copy(
            packed_ref.at[pl.ds(i * block, block)], out_ref.at[pl.ds(i * block, block)], leave.at[i]
        )
        for i in range(PARTS)
    ]
    for read in reads:
        read.start()
    target = target_ref[...]
    named = lax.broadcasted_iota(jnp.int32, (2 * chips, pairs), 0) == target
    earlier = jnp.dot(
        named.astype(jnp.bfloat16), strictly_before(pairs), preferred_element_type=jnp.float32
    )
    rank = jnp.sum(jnp.where(named, earlier, 0.0), axis=0, keepdims=True).astype(jnp.int32)
    slot = target * capacity + rank
    at_rank = (lax.broadcasted_iota(jnp.int32, (capacity, pairs), 0) == rank).astype(jnp.bfloat16)
    token = (lax.broadcasted_iota(jnp.int32, (1, pairs), 1) // chosen).astype(jnp.float32)
    gate = gate_ref[...]
    high = gate.astype(jnp.bfloat16).astype(jnp.float32)
    rest = gate - high
    middle = rest.astype(jnp.bfloat16).astype(jnp.float32)
    table_ref[...] = jnp.zeros(table_ref.shape, jnp.float32)
    for side in range(2):
        mine = 2 * lax.broadcasted_iota(jnp.int32, (chips, pairs), 0) + side == target
        for kind, value in enumerate((token, high, middle, rest - middle)):
            found = lax.dot_general(
                jnp.where(mine, value, 0.0).astype(jnp.bfloat16),
                at_rank,
                (((1,), (1,)), ((), ())),
                preferred_element_type=jnp.float32,
            )
            for copy in range(3) if kind == 0 else (kind - 1,):
                start = (2 * copy + side) * capacity
                table_ref[:, min(kind, 1), start : start + capacity] = found
    for i, read in enumerate(reads):
        read.wait()
        at = slice(i * rows, (i + 1) * rows)
        gate = raw_ref[at, :half].astype(jnp.float32)
        upper = raw_ref[at, half:].astype(jnp.float32)
        hidden_ref[at, :] = (gate / (1.0 + jnp.exp(-gate)) * upper).astype(jnp.bfloat16)
    slots = block * 2 * capacity
    for i, write in enumerate(writes):
        wanted = lax.broadcasted_iota(jnp.int32, (slots, pairs), 0) + i * slots
        picked = jnp.dot(
            (wanted == slot).astype(jnp.bfloat16),
            hidden_ref[...],
            preferred_element_type=jnp.float32,
        ).astype(jnp.bfloat16)
        for chip in range(block):
            for tile in range(half // 128):
                packed_ref[i * block + chip, tile * 2 * capacity : (tile + 1) * 2 * capacity, :] = (
                    picked[
                        chip * 2 * capacity : (chip + 1) * 2 * capacity,
                        tile * 128 : (tile + 1) * 128,
                    ]
                )
        packed_ref[i * block : (i + 1) * block, (half // 128) * 2 * capacity :, :] = table_ref[
            i * block : (i + 1) * block
        ].astype(jnp.bfloat16)
        write.start()
    for write in writes:
        write.wait()


def pack(target, gates, routed, chips, capacity, chosen):
    pairs, width = routed.shape
    tall = width // 256 * 2 * capacity + 8
    return pl.pallas_call(
        lambda *refs: pack_kernel(*refs, capacity=capacity, chosen=chosen),
        in_specs=[
            pl.BlockSpec(memory_space=pltpu.VMEM),
            pl.BlockSpec(memory_space=pltpu.VMEM),
            pl.BlockSpec(memory_space=pltpu.HBM),
        ],
        out_specs=pl.BlockSpec(memory_space=pltpu.HBM),
        out_shape=jax.ShapeDtypeStruct((chips, tall, 128), jnp.bfloat16),
        scratch_shapes=[
            pltpu.VMEM((pairs, width), jnp.bfloat16),
            pltpu.VMEM((pairs, width // 2), jnp.bfloat16),
            pltpu.VMEM((chips, 8, 128), jnp.float32),
            pltpu.VMEM((chips, tall, 128), jnp.bfloat16),
            pltpu.SemaphoreType.DMA((PARTS,)),
            pltpu.SemaphoreType.DMA((PARTS,)),
        ],
        compiler_params=pltpu.CompilerParams(vmem_limit_bytes=60 * 1024 * 1024),
        interpret=INTERPRET,
    )(target, gates, routed)


def expert_kernel(place_ref, *refs, count, capacity, start):
    packed = refs[:count]
    own_weight, other_weight, out_ref = refs[count : count + 3]
    tokens, wide = out_ref.shape[1:]
    core = place_ref[1]
    tiles = own_weight.shape[0] // 128
    reads = {}
    if start is not None:
        buffers, arrive = refs[count + 3 : count + 5], refs[count + 5]
        for i, (weight, buffer) in enumerate(zip((own_weight, other_weight), buffers)):
            reads[i] = pltpu.make_async_copy(
                weight.at[:, pl.ds(start, wide)], buffer, arrive.at[i]
            )
            reads[i].start()
        own_weight, other_weight = buffers

    def project(side, weight, read):
        blocks = [
            jnp.concatenate(
                [
                    p[0, pl.ds(pl.multiple_of((2 * t + side) * capacity, capacity), capacity), :]
                    for t in range(tiles)
                ],
                axis=1,
            )
            for p in packed
        ]
        rows = jnp.concatenate(blocks, axis=0)
        if read is not None:
            read.wait()
        return jnp.dot(rows, weight[...], preferred_element_type=jnp.float32).astype(jnp.bfloat16)

    own = project(core, own_weight, reads.get(0))
    other = project(1 - core, other_weight, reads.get(1))
    lower = jnp.where(core == 0, own, other)
    upper = jnp.where(core == 0, other, own)
    lanes = 4 * capacity
    wanted = lax.broadcasted_iota(jnp.int32, (tokens, lanes), 0).astype(jnp.float32)
    for i, p in enumerate(packed):
        at = slice(i * capacity, (i + 1) * capacity)
        stacked = jnp.concatenate([lower[at], upper[at]] * 2, axis=0)
        table = p[0, tiles * 2 * capacity :, :].astype(jnp.float32)
        scale = jnp.where(table[0:1, :lanes] == wanted, table[1:2, :lanes], 0.0).astype(jnp.bfloat16)
        out_ref[i] = jnp.dot(scale, stacked, preferred_element_type=jnp.float32).astype(
            jnp.bfloat16
        )


def expert_call(place, packed, own_weight, other_weight, homes, tokens, capacity, part, parts):
    chips, tall, _ = packed.shape
    width, columns = own_weight.shape
    columns = columns // parts
    steps = 4 if parts == 1 else 1
    piece = columns // steps
    count = len(homes)

    def row_spec(home):
        return pl.BlockSpec(
            (1, tall, 128), lambda j, s: (lax.rem(s[0] + (home + chips), chips), 0, 0)
        )

    if steps > 1:
        weight_spec = pl.BlockSpec((width, piece), lambda j, s: (0, j))
        start, scratch = None, []
    else:
        weight_spec = pl.BlockSpec(memory_space=pltpu.HBM)
        start = part * piece
        scratch = [pltpu.VMEM((width, piece), jnp.bfloat16)] * 2 + [pltpu.SemaphoreType.DMA((2,))]
    grid_spec = pltpu.PrefetchScalarGridSpec(
        num_scalar_prefetch=1,
        grid=(steps,),
        in_specs=[row_spec(h) for h in homes] + [weight_spec] * 2,
        out_specs=pl.BlockSpec((count, tokens, piece), lambda j, s: (0, 0, j)),
        scratch_shapes=scratch,
    )
    flops = 4 * count * capacity * width * columns
    return pl.pallas_call(
        lambda *refs: expert_kernel(*refs, count=count, capacity=capacity, start=start),
        grid_spec=grid_spec,
        out_shape=jax.ShapeDtypeStruct((count, tokens, columns), jnp.bfloat16),
        cost_estimate=pl.CostEstimate(
            flops=flops, bytes_accessed=4 * width * columns, transcendentals=0
        ),
        compiler_params=pltpu.CompilerParams(
            dimension_semantics=("arbitrary",), vmem_limit_bytes=48 * 1024 * 1024
        ),
        interpret=INTERPRET,
    )(place, *([packed] * count), own_weight, other_weight)


def add_kernel(left_ref, *refs):
    own, out_ref = refs[:-1], refs[-1]
    wide = out_ref.shape[1] // len(own)

    def some(i, carry):
        at = pl.ds(pl.multiple_of(i * 16, 16), 16)
        for n, right_ref in enumerate(own):
            to = slice(n * wide, (n + 1) * wide)
            total = left_ref[at, to].astype(jnp.float32) + right_ref[0, at].astype(jnp.float32)
            out_ref[at, to] = total.astype(jnp.bfloat16)
        return carry

    lax.fori_loop(0, out_ref.shape[0] // 16, some, 0)


def add_own(arrived, batches, place, at):
    whole = pl.BlockSpec(arrived.shape, lambda i: (0, 0))
    block = (1, arrived.shape[0], arrived.shape[1] // len(batches))
    return pl.pallas_call(
        add_kernel,
        grid=(1,),
        in_specs=[whole]
        + [pl.BlockSpec(block, lambda i: (place, 0, at)) for _ in batches],
        out_specs=whole,
        out_shape=jax.ShapeDtypeStruct(arrived.shape, jnp.bfloat16),
        compiler_params=pltpu.CompilerParams(vmem_limit_bytes=4 * 1024 * 1024),
        interpret=INTERPRET,
    )(arrived, *batches)


def on_device(expert_ids, route_gates, routed_in, down_weight, slot_offset):
    experts = lax.axis_size("ep")
    chips = experts // 2
    tokens, chosen = expert_ids.shape
    pairs = tokens * chosen
    capacity = 2 * pairs // experts
    weight = down_weight[0]
    index = lax.axis_index("ep")
    place = jnp.stack([index // 2, lax.rem(index, 2)]).astype(jnp.int32)

    def shifted(value, distance):
        return lax.ppermute(
            value, "ep", [(i, (i + 2 * distance) % experts) for i in range(experts)]
        )

    target = jnp.mod(expert_ids - slot_offset[0], experts).reshape(1, pairs)
    packed = pack(
        target,
        route_gates.reshape(1, pairs),
        routed_in.reshape(pairs, routed_in.shape[2]),
        chips,
        capacity,
        chosen,
    )
    same_core = [[2 * z + c for z in range(chips)] for c in range(2)]
    other_weight = lax.ppermute(weight, "ep", [(i, i ^ 1) for i in range(experts)])
    packed = lax.all_to_all(
        packed,
        "ep",
        split_axis=0,
        concat_axis=0,
        axis_index_groups=same_core,
        tiled=True,
    )


    half = chips // 2
    sums = {}
    first = 0
    for count, pieces in zip(STEPS, PIECES):
        steps = range(first, first + count)
        first += count
        homes = [half - s for s in steps] + [s + 1 - half for s in steps]
        batches = []
        for piece in range(pieces):
            batches.append(
                expert_call(
                    place,
                    packed,
                    weight,
                    other_weight,
                    homes,
                    tokens,
                    capacity,
                    piece,
                    pieces,
                )
            )
        for i, home in enumerate(homes):
            for c in range(CHAINS):
                if pieces < CHAINS:
                    sums[home, c] = (batches, i, c)
                else:
                    each = pieces // CHAINS
                    sums[home, c] = (batches[c * each : (c + 1) * each], i, 0)

    def own_sum(home, c):
        batches, i, at = sums[home, c]
        wide = weight.shape[1] // CHAINS // len(batches)
        return jnp.concatenate(
            [batch[i, :, at * wide : (at + 1) * wide] for batch in batches], axis=1
        )

    def with_own(arrived, home, c):
        return add_own(arrived, *sums[home, c])

    ahead = [own_sum(half, c) for c in range(CHAINS)]
    behind = [own_sum(1 - half, c) for c in range(CHAINS)]
    for step in range(half):
        for c in range(CHAINS):
            ahead[c] = shifted(ahead[c], 1)
            if step < half - 1:
                behind[c] = shifted(behind[c], -1)
                ahead[c] = with_own(ahead[c], half - 1 - step, c)
            if step < half - 2:
                behind[c] = with_own(behind[c], step + 2 - half, c)
    return jnp.concatenate(
        [
            (
                ahead[c].astype(jnp.float32)
                + behind[c].astype(jnp.float32)
                + own_sum(0, c).astype(jnp.float32)
            ).astype(jnp.bfloat16)
            for c in range(CHAINS)
        ],
        axis=1,
    )


def solution(mesh):
    placed = (
        P(("grp", "ep"), None),
        P(("grp", "ep"), None),
        P(("grp", "ep"), None, None),
        P("ep", None, None),
        P(),
    )
    return jax.shard_map(
        on_device, mesh=mesh, in_specs=placed, out_specs=P(("grp", "ep"), None), check_vma=False
    )
```
